8 devices in a mesh: data: 8 (over z, y, x, core).
Axes of the slice: x: 2, y: 2, z: 1, core: 2. Of those that a mesh axis runs over, the one named last changes fastest.
Arguments:
- grad_qkv: bfloat16 [8, 3, 3145728], P('data')
- weight_qkv: float32 [3, 3145728], P(None, 'data')
- mom_qkv: float32 [3, 3145728], P(None, 'data')
- var_qkv: float32 [3, 3145728], P(None, 'data')
- grad_proj: bfloat16 [8, 3, 1048576], P('data')
- weight_proj: float32 [3, 1048576], P(None, 'data')
- mom_proj: float32 [3, 1048576], P(None, 'data')
- var_proj: float32 [3, 1048576], P(None, 'data')
- grad_fc_in: bfloat16 [8, 3, 4194304], P('data')
- weight_fc_in: float32 [3, 4194304], P(None, 'data')
- mom_fc_in: float32 [3, 4194304], P(None, 'data')
- var_fc_in: float32 [3, 4194304], P(None, 'data')
- grad_fc_out: bfloat16 [8, 3, 4194304], P('data')
- weight_fc_out: float32 [3, 4194304], P(None, 'data')
- mom_fc_out: float32 [3, 4194304], P(None, 'data')
- var_fc_out: float32 [3, 4194304], P(None, 'data')
Outputs:
- output 1: bfloat16 [3, 3145728], replicated
- output 2: float32 [3, 3145728], P(None, 'data')
- output 3: float32 [3, 3145728], P(None, 'data')
- output 4: float32 [3, 3145728], P(None, 'data')
- output 5: bfloat16 [3, 1048576], replicated
- output 6: float32 [3, 1048576], P(None, 'data')
- output 7: float32 [3, 1048576], P(None, 'data')
- output 8: float32 [3, 1048576], P(None, 'data')
- output 9: bfloat16 [3, 4194304], replicated
- output 10: float32 [3, 4194304], P(None, 'data')
- output 11: float32 [3, 4194304], P(None, 'data')
- output 12: float32 [3, 4194304], P(None, 'data')
- output 13: bfloat16 [3, 4194304], replicated
- output 14: float32 [3, 4194304], P(None, 'data')
- output 15: float32 [3, 4194304], P(None, 'data')
- output 16: float32 [3, 4194304], P(None, 'data')
All inputs are finite; a program needn't handle non-finite values.
Results may differ from the reference program's by a relative error of at most 0.001.
Values are sent between devices in bfloat16 or wider.
A program may use at most 1 GiB of HBM per device.

```python
import jax
import jax.numpy as jnp

D = 1024
FF = 4096
LAYERS = 3
DATA = 8
STEP = 10

LEARN_RATE = 0.1
BETA_ONE = 0.9
BETA_TWO = 0.999
EPSILON = 1e-6
WEIGHT_DECAY = 0.01
TENSOR_SHAPES = ((D, 3 * D), (D, D), (D, FF), (FF, D))
KIND_NAMES = ("qkv", "proj", "fc_in", "fc_out")


def draw_tensor(rng_key, fan_in, fan_out):
    size_flat = fan_in * fan_out
    sub_keys = jax.random.split(rng_key, 8)
    position = jnp.arange(size_flat, dtype=jnp.float32) / size_flat - 0.5
    sign_flip = 2.0 * jax.random.randint(sub_keys[0], (LAYERS, 1), 0, 2).astype(jnp.float32) - 1.0
    ramp_slope = sign_flip * jax.random.uniform(sub_keys[1], (LAYERS, 1), minval=1.0, maxval=2.0)
    weight_scale = fan_in ** -0.5 * jnp.exp(jax.random.uniform(sub_keys[2], (LAYERS, 1), minval=-1.0, maxval=1.0))
    grad_scale = 10.0 * jnp.exp(jax.random.uniform(sub_keys[3], (LAYERS, 1), minval=-1.0, maxval=1.0))
    weight = weight_scale * jnp.exp(ramp_slope * position) * jax.random.normal(sub_keys[4], (LAYERS, size_flat))
    local_grad = grad_scale * DATA ** 0.5 * jax.random.normal(sub_keys[5], (DATA, LAYERS, size_flat))
    first_mom = 0.05 * grad_scale * jax.random.normal(sub_keys[6], (LAYERS, size_flat))
    second_mom = 0.0005 * grad_scale * grad_scale * jax.random.uniform(sub_keys[7], (LAYERS, size_flat), minval=0.5, maxval=1.5)
    return local_grad.astype(jnp.bfloat16), weight, first_mom, second_mom


def setup_inputs(seed: int = 0) -> dict:
    root_key = jax.random.key(seed)
    arrays = {}
    for kind_pos in range(4):
        fan_in, fan_out = TENSOR_SHAPES[kind_pos]
        drawn_set = draw_tensor(jax.random.fold_in(root_key, kind_pos), fan_in, fan_out)
        arrays["grad_" + KIND_NAMES[kind_pos]] = drawn_set[0]
        arrays["weight_" + KIND_NAMES[kind_pos]] = drawn_set[1]
        arrays["mom_" + KIND_NAMES[kind_pos]] = drawn_set[2]
        arrays["var_" + KIND_NAMES[kind_pos]] = drawn_set[3]
    return arrays


def lamb_tensor(local_grad, weight, first_mom, second_mom):
    grad_mean = jnp.sum(local_grad, axis=0, dtype=jnp.float32) / local_grad.shape[0]
    new_first = BETA_ONE * first_mom + (1.0 - BETA_ONE) * grad_mean
    new_second = BETA_TWO * second_mom + (1.0 - BETA_TWO) * grad_mean * grad_mean
    direction = (new_first / (1.0 - BETA_ONE ** STEP)) / (jnp.sqrt(new_second / (1.0 - BETA_TWO ** STEP)) + EPSILON) + WEIGHT_DECAY * weight
    weight_norm = jnp.sqrt(jnp.sum(weight * weight, axis=1, keepdims=True))
    update_norm = jnp.sqrt(jnp.sum(direction * direction, axis=1, keepdims=True))
    new_weight = weight - LEARN_RATE * (weight_norm / update_norm) * direction
    return new_weight.astype(jnp.bfloat16), new_weight, new_first, new_second


def reference(grad_qkv, weight_qkv, mom_qkv, var_qkv, grad_proj, weight_proj, mom_proj, var_proj, grad_fc_in, weight_fc_in, mom_fc_in, var_fc_in, grad_fc_out, weight_fc_out, mom_fc_out, var_fc_out):
    copy_qkv, new_weight_qkv, new_mom_qkv, new_var_qkv = lamb_tensor(grad_qkv, weight_qkv, mom_qkv, var_qkv)
    copy_proj, new_weight_proj, new_mom_proj, new_var_proj = lamb_tensor(grad_proj, weight_proj, mom_proj, var_proj)
    copy_fc_in, new_weight_fc_in, new_mom_fc_in, new_var_fc_in = lamb_tensor(grad_fc_in, weight_fc_in, mom_fc_in, var_fc_in)
    copy_fc_out, new_weight_fc_out, new_mom_fc_out, new_var_fc_out = lamb_tensor(grad_fc_out, weight_fc_out, mom_fc_out, var_fc_out)
    return (copy_qkv, new_weight_qkv, new_mom_qkv, new_var_qkv, copy_proj, new_weight_proj, new_mom_proj, new_var_proj, copy_fc_in, new_weight_fc_in, new_mom_fc_in, new_var_fc_in, copy_fc_out, new_weight_fc_out, new_mom_fc_out, new_var_fc_out)
```

```python
import jax
import jax.numpy as jnp
from jax import lax
from jax.sharding import PartitionSpec as P

STEP = 10
LEARN_RATE = 0.1
BETA_ONE = 0.9
BETA_TWO = 0.999
EPSILON = 1e-6
WEIGHT_DECAY = 0.01


def flip(bit):
    return [(i, i ^ bit) for i in range(8)]


def swap(value, bit):
    return lax.ppermute(value, "data", flip(bit))


def pick(value, index, axis):
    return lax.dynamic_slice_in_dim(value, index, 1, axis)


def solution(mesh):
    grad_spec = P("data", None, None)
    shard_spec = P(None, "data")
    full_spec = P(None, None)

    def device_step(*blocks):
        me = lax.axis_index("data")
        core, col, row = me % 2, (me // 2) % 2, me // 4
        kinds = [blocks[4 * k:4 * k + 4] for k in range(4)]
        order = [1, 0, 2, 3]
        f32 = jnp.float32

        def repack(piece):
            return jnp.transpose(piece[:, :, :, :, 0], (1, 2, 3, 0, 4, 5))

        state = {}
        for k in order:
            grad = kinds[k][0]
            n = grad.shape[2]
            rows = n // 2048
            view = grad.reshape(3, 2, 2, 2, 2, rows, 128)
            half_a, half_b = view[:, :, :, :, 0:1], view[:, :, :, :, 1:2]
            send_a = repack(pick(half_a, 1 - col, 2))
            send_b = repack(pick(half_b, 1 - row, 1))
            keep_a = repack(pick(half_a, col, 2))
            keep_b = repack(pick(half_b, row, 1))
            got_a = swap(send_a, 2)
            got_b = swap(send_b, 4)
            state[k] = (keep_a, got_a, keep_b, got_b)
        sums = {}
        for k in order:
            keep_a, got_a, keep_b, got_b = state[k]

            def part(keep, got, c):
                return pick(keep, c, 2).astype(f32) + pick(got, c, 2).astype(f32)
            far_a = swap(part(keep_a, got_a, 1 - core), 1)
            far_b = swap(part(keep_b, got_b, 1 - core), 1)
            near_a = part(keep_a, got_a, core) + far_a
            near_b = part(keep_b, got_b, core) + far_b
            sums[k] = (near_a, near_b)
        out = [None] * 16
        copies = {}
        for k in order:
            near_a, near_b = sums[k]
            last_a = swap(pick(near_a, 1 - row, 0), 4)
            last_b = swap(pick(near_b, 1 - col, 1), 2)
            total_a = (pick(near_a, row, 0) + last_a)[0, 0, 0]
            total_b = (pick(near_b, col, 1) + last_b)[0, 0, 0]
            total = jnp.concatenate([total_a, total_b], axis=1)
            _, weight, mom, var = kinds[k]
            grad_mean = total.reshape(weight.shape) / 8
            new_first = BETA_ONE * mom + (1.0 - BETA_ONE) * grad_mean
            new_second = BETA_TWO * var + (1.0 - BETA_TWO) * grad_mean * grad_mean
            direction = (new_first / (1.0 - BETA_ONE ** STEP)) / (jnp.sqrt(new_second / (1.0 - BETA_TWO ** STEP)) + EPSILON) + WEIGHT_DECAY * weight
            part_sums = jnp.stack([jnp.sum(weight * weight, axis=1), jnp.sum(direction * direction, axis=1)])
            for bit in (1, 2, 4):
                part_sums = part_sums + swap(part_sums, bit)
            norm_pair = jnp.sqrt(part_sums)
            ratio = (norm_pair[0] / norm_pair[1])[:, None]
            new_weight = weight - LEARN_RATE * ratio * direction
            out[4 * k + 1:4 * k + 4] = [new_weight, new_first, new_second]
            own = new_weight.astype(jnp.bfloat16).reshape(3, -1, 128)
            copies[k] = own
        for k in order:
            own = copies[k]
            half = own.shape[1] // 2
            by_x = swap(own, 2)
            by_y = swap(own, 4)
            diag = jnp.concatenate([swap(by_x[:, :half], 4), swap(by_y[:, half:], 2)], axis=1)
            mine = [own, by_x, by_y, diag]
            theirs = [swap(v, 1) for v in mine]
            full = jnp.zeros((8,) + own.shape, own.dtype)
            for j in range(4):
                for c, val in ((0, mine[j]), (1, theirs[j])):
                    full = lax.dynamic_update_slice_in_dim(full, val[None], me ^ (2 * j + c), 0)
            out[4 * k] = jnp.transpose(full, (1, 0, 2, 3)).reshape(3, -1)
        return tuple(out)

    return jax.shard_map(device_step, mesh=mesh, in_specs=(grad_spec, shard_spec, shard_spec, shard_spec) * 4, out_specs=(full_spec, shard_spec, shard_spec, shard_spec) * 4, check_vma=False)
```
